32 devices in a mesh: dp: 4 (over y, core), fsdp: 8 (over z, x).
Axes of the slice: x: 2, y: 2, z: 4, core: 2. Of those that a mesh axis runs over, the one named last changes fastest.
Arguments:
- data_samples: bfloat16 [512, 4096], P('dp', 'fsdp'), may hold values from -6 to 6
- negative_start: float32 [512, 4096], P('dp', 'fsdp'), may hold values from -6 to 6
- langevin_noise: float32 [4, 512, 4096], P(None, 'dp', 'fsdp'), may hold values from -6 to 6
- first_weight: bfloat16 [4096, 4096], P('fsdp'), may hold values from -0.09375 to 0.09375
- second_weight: bfloat16 [4096, 4096], P('fsdp'), may hold values from -0.09375 to 0.09375
- readout: float32 [4096], P('fsdp'), may hold values from -480 to 480
Outputs:
- first_grad: float32 [4096, 4096], P('fsdp', 'dp')
- second_grad: float32 [4096, 4096], P('fsdp', 'dp')
- energy_gap: float32 [], replicated
The draws below stay inside these ranges and needn't reach their ends.
All inputs are finite; a program needn't handle non-finite values.
Results may differ from the reference program's by a relative error of at most 0.014.
Values may be sent and summed in bfloat16 or wider, within the bound.
A program may use at most 64 MiB of HBM per device.

```python
import jax
import jax.numpy as jnp
from jax import lax

D = 4096
H = 4096
STEPS = 4
SAMPLES = 512
N_FSDP = 8


def levels(own_key, shape, cuts, least, high):
    level = 1.0
    for axis_at, shards_of in cuts:
        heights = jax.random.uniform(jax.random.fold_in(jax.random.fold_in(own_key, 6), axis_at), (shards_of,), jnp.float32, least / len(cuts), high / len(cuts))
        level = level * jnp.repeat(jnp.exp(heights), shape[axis_at] // shards_of).reshape((-1,) + (1,) * (len(shape) - 1 - axis_at))
    return level


def bell_draw(rng, extent, spread, most, cuts=(), kind=jnp.bfloat16):
    entries = jax.random.normal(rng, extent, jnp.float32) * spread
    if len(cuts) > 0:
        entries = levels(rng, extent, cuts, -0.22, 0.18) * entries
    return jnp.clip(entries, min=-most, max=most).astype(kind)


def setup_inputs(seed: int = 0) -> dict:
    arg_keys = jax.random.split(jax.random.key(seed), 7)
    return {
        "data_samples": bell_draw(arg_keys[0], (SAMPLES, D), 1.0, 6.0, ((0, 4), (1, 8))),
        "negative_start": bell_draw(arg_keys[1], (SAMPLES, D), 1.0, 6.0, ((0, 4), (1, 8)), jnp.float32),
        "langevin_noise": bell_draw(arg_keys[2], (STEPS, SAMPLES, D), 1.0, 6.0, ((1, 4), (2, 8)), jnp.float32),
        "first_weight": bell_draw(arg_keys[3], (D, H), D ** -0.5, 0.09375, ((0, 8),)),
        "second_weight": bell_draw(arg_keys[4], (H, H), H ** -0.5, 0.09375, ((0, 8),)),
        "readout": bell_draw(arg_keys[5], (H,), 80.0, 480.0, ((0, 8),), jnp.float32),
    }


def slope(values):
    sig = jax.nn.sigmoid(values)
    return sig * (1.0 + values * (1.0 - sig))

def layer(inputs, weight):
    count = inputs.shape[0]
    width = weight.shape[0]
    pieces = jnp.einsum('rnk,nkh->nrh', inputs.reshape(count, N_FSDP, width // N_FSDP).astype(jnp.float32), weight.reshape(N_FSDP, width // N_FSDP, weight.shape[1]).astype(jnp.float32), precision=lax.Precision.HIGHEST)
    rounded = lax.optimization_barrier(pieces.astype(jnp.bfloat16))
    return lax.optimization_barrier(jnp.sum(rounded.astype(jnp.float32), axis=0))

def forward(inputs, first_weight, second_weight):
    pre_one = layer(inputs, first_weight)
    hidden = jax.nn.silu(pre_one).astype(jnp.bfloat16)
    pre_two = layer(hidden, second_weight)
    return (pre_one, hidden, pre_two)

def backward(cotan, readout, pre_one, pre_two, second_weight):
    grad_two = (cotan[:, None] * readout[None, :] * slope(pre_two)).astype(jnp.bfloat16)
    back_one = jnp.dot(grad_two, second_weight.T, preferred_element_type=jnp.float32)
    grad_one = (back_one * slope(pre_one)).astype(jnp.bfloat16)
    return (grad_two, grad_one)

def reference(data_samples, negative_start, langevin_noise, first_weight, second_weight, readout):
    state = negative_start
    ones = jnp.ones((state.shape[0],), jnp.float32)
    for step in range(STEPS):
        inputs = state.astype(jnp.bfloat16)
        pre_one, hidden, pre_two = forward(inputs, first_weight, second_weight)
        grad_two, grad_one = backward(ones, readout, pre_one, pre_two, second_weight)
        moved = jnp.dot(grad_one, first_weight.T, preferred_element_type=jnp.float32)
        state = state - 0.005 * moved + 0.1 * langevin_noise[step]
    rows = jnp.concatenate([data_samples, state.astype(jnp.bfloat16)], axis=0)
    cotan = jnp.concatenate([ones, -ones])
    pre_one, hidden, pre_two = forward(rows, first_weight, second_weight)
    energies = jnp.dot(jax.nn.silu(pre_two), readout, precision=lax.Precision.HIGHEST)
    energy_gap = jnp.sum(cotan * energies) / (SAMPLES * 80.0 * jnp.sqrt(jnp.float32(H)))
    grad_two, grad_one = backward(cotan, readout, pre_one, pre_two, second_weight)
    raw_one = jnp.dot(rows.T, grad_one, preferred_element_type=jnp.float32)
    raw_two = jnp.dot(hidden.T, grad_two, preferred_element_type=jnp.float32)
    total = jnp.sum(raw_one * raw_one) + jnp.sum(raw_two * raw_two)
    scale = jnp.sqrt(total / (2.0 * D * H) + 1e-06)
    return (raw_one / scale, raw_two / scale, energy_gap)
```

```python
import functools

import jax
import jax.numpy as jnp
from jax import lax
from jax.experimental import pallas as pl
from jax.experimental.pallas import tpu as pltpu
from jax.sharding import PartitionSpec as P

MESH = pl.DeviceIdType.MESH
BF16 = jnp.bfloat16
F32 = jnp.float32
PIECES = 4


def inner_of(n):
    return max(i for i in range(1, n + 1) if n % i == 0 and i * i <= n)


def folded(values):
    rows, columns = values.shape
    tall = values.reshape(rows // 8, 8, columns).sum(axis=0)
    out = tall[:, :128]
    for at in range(128, columns, 128):
        out += tall[:, at : at + 128]
    return out


def kernel(
    n, X, dpn, steps, S,
    data_ref, start_ref, noise_in, w1_ref, w2_ref, read_ref,
    raw1_ref, raw2_ref, stat_ref,
    wm1, wm2, state, noise, u_own, hid, slope_1, acc, tot, read_all,
    s_a, r_a, s_b, r_b, buf, rows_all, hid_all, g_all, energy, own_stat, got_stat,
    sem_l, sem_is, sem_ir, sem_rs, sem_rr, sem_wzs, sem_wzr, sem_wys, sem_wyr, sem_wcs, sem_wcr,
    sem_as, sem_ar, sem_bs, sem_br, sem_zs, sem_zr, sem_xs, sem_xr, sem_ds, sem_dr, sem_ts, sem_tr,
):
    Z = n // X
    K = Z // 2
    Y = dpn // 2
    T = 2 * S
    q = n // dpn
    C = w1_ref.shape[0]
    H = w1_ref.shape[1]
    h = state.shape[1]
    slice_rows = C // dpn
    piece = H // PIECES
    me = lax.axis_index("fsdp")
    dpi = lax.axis_index("dp")
    z, x = me // X, me % X
    k, a = z // 2, z % 2
    y, c = dpi // 2, dpi % 2
    other = 1 - a
    self_at = k * X + x

    def device(kd, ad, xd):
        return (kd * 2 + ad) * X + xd

    def x_peer(ox):
        return device(k, a, (x + ox) % X)

    def k_peer(ok):
        return device((k + ok) % K, a, x)

    def z_peer(oz):
        return ((z + oz) % Z) * X + x

    def dp_peer(o):
        return (dpi + o) % dpn

    def half_cols(at):
        return pl.ds(pl.multiple_of(at * C, C), C)

    def shard_cols(kd, i, xd):
        return pl.ds(pl.multiple_of(device(kd, i, xd) * C, C), C)

    def send(src, dst, ssem, rsem, peer):
        return pltpu.make_async_remote_copy(
            src_ref=src, dst_ref=dst, send_sem=ssem, recv_sem=rsem, device_id=peer, device_id_type=MESH
        )

    def fetch(src, dst, sem):
        return pltpu.make_async_copy(src, dst, sem)

    offsets = [(oa, od) for oa in range(2) for od in range(dpn) if (oa, od) != (0, 0)]

    def swap_peer(oa, od):
        return {"fsdp": device(k, (a + oa) % 2, x), "dp": dp_peer(od)}

    partners = (
        [{"fsdp": x_peer(ox)} for ox in range(1, X)]
        + [{"fsdp": z_peer(oz)} for oz in range(1, Z)]
        + [swap_peer(oa, od) for oa, od in offsets if od]
    )
    barrier = pltpu.get_barrier_semaphore()
    for peer in partners:
        pl.semaphore_signal(barrier, inc=1, device_id=peer, device_id_type=MESH)
    pl.semaphore_wait(barrier, len(partners))

    partner = {"fsdp": device(k, other, x)}

    def rows_in(half, s):
        return pl.ds(pl.multiple_of((half * S + s) * h, h), h)

    def pieces_in(kind, s, half, slot):
        if kind == 0:
            return data_ref.at[rows_in(half, s), :], u_own.at[S + s, :, half_cols(slot)]
        if kind == 1:
            return start_ref.at[rows_in(half, s), :], state.at[s, :, half_cols(slot)]
        return noise_in.at[:, rows_in(half, s), :], noise.at[:, s, :, half_cols(slot)]

    def keep_in(kind, s):
        src, dst = pieces_in(kind, s, a, a)
        return fetch(src, dst, sem_l.at[kind * S + s])

    def give_in(kind, s, slot):
        src, dst = pieces_in(kind, s, other, slot)
        return send(src, dst, sem_is.at[kind, s], sem_ir.at[kind, s], partner)

    def read_copy(oz, at):
        return send(read_ref, read_all.at[at], sem_rs.at[oz - 1], sem_rr.at[oz - 1], {"fsdp": z_peer(oz)})

    weights = ((w1_ref, wm1), (w2_ref, wm2))

    def keep_w(w):
        src, dst = weights[w]
        return fetch(src, dst.at[half_cols(a), :], sem_l.at[3 * S + w])

    def w_rows(slot, d):
        return pl.ds(pl.multiple_of(slot * C + d * slice_rows, slice_rows), slice_rows)

    def w_cols(p):
        return pl.ds(p * piece, piece)

    def wz_copy(w, p, slot):
        src, dst = weights[w]
        return send(
            src.at[w_rows(0, dpi), w_cols(p)], dst.at[w_rows(slot, dpi), w_cols(p)],
            sem_wzs.at[w, p], sem_wzr.at[w, p], partner,
        )

    def wy_copy(w, p, o, d):
        ref = weights[w][1].at[w_rows(other, d), w_cols(p)]
        return send(
            ref, ref, sem_wys.at[w, p, o - 1], sem_wyr.at[w, p, o - 1], {"dp": ((y + o) % Y) * 2 + c}
        )

    def wc_copy(w, p, o, d):
        ref = weights[w][1].at[w_rows(other, d), w_cols(p)]
        return send(ref, ref, sem_wcs.at[w, p, o], sem_wcr.at[w, p, o], {"dp": y * 2 + 1 - c})

    def y_source(o):
        return (y + Y - o) % Y

    def weight_steps(w):
        for p in range(PIECES + 1):
            if p < PIECES:
                wz_copy(w, p, other).wait_recv()
                for o in range(1, Y):
                    wy_copy(w, p, o, dpi).start()
                wc_copy(w, p, 0, dpi).start()
            if p:
                for o in range(1, Y):
                    d = y_source(o) * 2 + c
                    wy_copy(w, p - 1, o, d).wait_recv()
                    wc_copy(w, p - 1, o, d).start()
            yield
        for p in range(PIECES):
            for o in range(Y):
                wc_copy(w, p, o, y_source(o) * 2 + 1 - c).wait_recv()
        keep_w(w).wait()

    def weight_settle(w):
        for p in range(PIECES):
            wz_copy(w, p, a).wait_send()
            for o in range(1, Y):
                wy_copy(w, p, o, dpi).wait_send()
            for o in range(Y):
                wc_copy(w, p, o, dpi).wait_send()

    def a_copy(s, j, ok, ox):
        return send(
            s_a.at[s, j, ok, ox - 1], r_a.at[s, j, ok, ox - 1],
            sem_as.at[s, j, ok, ox - 1], sem_ar.at[s, j, ok, ox - 1], {"fsdp": x_peer(ox)},
        )

    def b_copy(s, j, ok, part):
        at = 0 if j == 0 else 1 + part
        return send(
            s_b.at[s, ok - 1 if j == 0 else K - 1 + part], r_b.at[s, ok - 1, at],
            sem_bs.at[s, ok - 1, at], sem_br.at[s, ok - 1, at], {"fsdp": k_peer(ok)},
        )

    order = list(range(1, K)) + [0]

    def two_dots(lhs, w, kd, xd):
        return [
            jnp.dot(lhs, w[:, shard_cols(kd, i, xd)], preferred_element_type=F32) for i in range(2)
        ]

    def scatter_open(s, j, lhs, w):
        for ok in order:
            for ox in range(1, X):
                for i, part in enumerate(two_dots(lhs, w, (k + ok) % K, (x + ox) % X)):
                    s_a[s, j, ok, ox - 1, :, i * C : (i + 1) * C] = part.astype(BF16)
                a_copy(s, j, ok, ox).start()
        for ok in order:
            for i, part in enumerate(two_dots(lhs, w, (k + ok) % K, x)):
                acc[s, ok, :, i * C : (i + 1) * C] = part

    def joined(s, j, ok):
        total = acc[s, ok]
        for ox in range(1, X):
            a_copy(s, j, ok, ox).wait_recv()
            total += r_a[s, j, ok, ox - 1].astype(F32)
        return total

    def open_1(s):
        scatter_open(s, 0, u_own[s], wm1)

    def join_1(s):
        for ok in range(1, K):
            s_b[s, ok - 1] = joined(s, 0, ok).astype(BF16)
            b_copy(s, 0, ok, 0).start()

    def close_1(s):
        a1 = joined(s, 0, 0)
        for ok in range(1, K):
            b_copy(s, 0, ok, 0).wait_recv()
            a1 += r_b[s, ok - 1, 0].astype(F32)
        s1 = jax.nn.sigmoid(a1)
        hid[s] = (a1 * s1).astype(BF16)
        slope_1[s] = s1 * (1.0 + a1 * (1.0 - s1))
        scatter_open(s, 1, hid[s], wm2)

    def join_2(s):
        for ok in order:
            total = joined(s, 1, ok)
            acc[s, ok] = total
            s_b[s, K - 1 + ok] = total.astype(BF16)
            for to in range(1, K):
                b_copy(s, 1, to, ok).start()

    def x_copy(s, stage, ok, ox, at):
        ref = buf.at[s, stage, at]
        return send(
            ref, ref, sem_xs.at[s, stage, ok, ox - 1], sem_xr.at[s, stage, ok, ox - 1], {"fsdp": x_peer(ox)}
        )

    def z_copy(s, ok, at):
        ref = buf.at[s, 1, at]
        return send(ref, ref, sem_zs.at[s, ok - 1], sem_zr.at[s, ok - 1], {"fsdp": k_peer(ok)})

    def block(s, stage, kd, xd, w):
        total = None
        for i in range(2):
            part = lax.dot_general(
                buf[s, stage, kd * X + xd, :, i * C : (i + 1) * C], w[:, shard_cols(kd, i, xd)],
                (((1,), (1,)), ((), ())), preferred_element_type=F32,
            )
            total = part if total is None else total + part
        return total

    def close_2(s, sign):
        for ok in order:
            kd = (k + ok) % K
            a2 = acc[s, ok]
            for frm in range(1, K):
                part = (ok + frm) % K
                b_copy(s, 1, frm, part).wait_recv()
                a2 += r_b[s, frm - 1, 1 + part].astype(F32)
            gain = jnp.concatenate([read_all[kd * 2], read_all[kd * 2 + 1]], axis=1)
            s2 = jax.nn.sigmoid(a2)
            buf[s, 0, kd * X + x] = (sign * gain * (s2 * (1.0 + a2 * (1.0 - s2)))).astype(BF16)
            for ox in range(1, X):
                x_copy(s, 0, ok, ox, kd * X + x).start()
            if ok == 0:
                energy[s] = folded(gain * (a2 * s2))
        total = None
        for ok in order:
            part = block(s, 0, (k + ok) % K, x, wm2)
            total = part if total is None else total + part
        tot[s] = total

    def back_2(s):
        total = tot[s]
        for ok in order:
            for ox in range(1, X):
                kd, xd = (k + ok) % K, (x + X - ox) % X
                x_copy(s, 0, ok, ox, kd * X + xd).wait_recv()
                total += block(s, 0, kd, xd, wm2)
        buf[s, 1, self_at] = (total * slope_1[s]).astype(BF16)
        for ok in range(1, K):
            z_copy(s, ok, self_at).start()
        for ox in range(1, X):
            x_copy(s, 1, 0, ox, self_at).start()

    def forward_1(s, moving):
        if moving:
            total = block(s, 1, k, x, wm1)
        for ok in range(1, K):
            kd = (k + K - ok) % K
            z_copy(s, ok, kd * X + x).wait_recv()
            for ox in range(1, X):
                x_copy(s, 1, ok, ox, kd * X + x).start()
            if moving:
                total += block(s, 1, kd, x, wm1)
        if moving:
            tot[s] = total

    def back_1(s, moving):
        if moving:
            total = tot[s]
        for ok in range(K):
            for ox in range(1, X):
                kd, xd = (k + K - ok) % K, (x + X - ox) % X
                x_copy(s, 1, ok, ox, kd * X + xd).wait_recv()
                if moving:
                    total += block(s, 1, kd, xd, wm1)
        if moving:
            return total

    def settle(s):
        for j in range(2):
            for ok in range(K):
                for ox in range(1, X):
                    a_copy(s, j, ok, ox).wait_send()
                    x_copy(s, j, ok, ox, self_at).wait_send()
        for ok in range(1, K):
            b_copy(s, 0, ok, 0).wait_send()
            for part in range(K):
                b_copy(s, 1, ok, part).wait_send()
            z_copy(s, ok, self_at).wait_send()

    def place(half, kind, p, s):
        if kind == 0:
            return rows_all.at[half, p, s]
        if kind == 1:
            return hid_all.at[half, p, s]
        return g_all.at[half, (kind - 2) // q, (kind - 2) % q, p, s]

    def source(half, kind, s, ad, dd):
        at = s if half else S + s
        if kind == 0:
            return u_own.at[at, :, half_cols(ad)]
        if kind == 1:
            return hid.at[at, :, half_cols(ad)]
        stage, i = (kind - 2) // q, (kind - 2) % q
        shard = dd * q + i
        zd, xd = shard // X, shard % X
        return buf.at[at, stage, (zd // 2) * X + xd, :, half_cols(zd % 2)]

    mine = a * dpn + dpi

    def swap(half, kind, e, s, p):
        oa, od = offsets[e]
        return send(
            source(half, kind, s, (a + oa) % 2, dp_peer(od)), place(half, kind, p, s),
            sem_ds.at[half, kind, e, s], sem_dr.at[half, kind, e, s], swap_peer(oa, od),
        )

    def exchange(half, kinds, s):
        for kind in kinds:
            for e in range(len(offsets)):
                swap(half, kind, e, s, mine).start()
        for kind in kinds:
            place(half, kind, mine, s)[...] = source(half, kind, s, a, dpi)[...]

    def arrived(half, kinds):
        def one(s):
            for kind in kinds:
                for e, (oa, od) in enumerate(offsets):
                    p = ((a + oa) % 2) * dpn + (dpi + dpn - od) % dpn
                    swap(half, kind, e, s, p).wait_recv()

        each(0, S, one)

    def exchange_settle(half):
        def one(s):
            for kind in range(2 + 2 * q):
                for e in range(len(offsets)):
                    swap(half, kind, e, s, mine).wait_send()

        each(0, S, one)

    def each(low, high, stage, *args):
        def body(s, carry):
            stage(s, *args)
            return carry

        lax.fori_loop(low, high, body, 0)

    first_kinds, last_kinds = [2 + i for i in range(q)], [2 + q + i for i in range(q)]

    for s in range(S):
        give_in(1, s, a).start()
        give_in(0, s, a).start()
    for w in range(2):
        for p in range(PIECES):
            wz_copy(w, p, a).start()
    for oz in range(1, Z):
        read_copy(oz, z).start()
    for s in range(S):
        keep_in(1, s).start()
        keep_in(0, s).start()
    for w in range(2):
        keep_w(w).start()
    for s in range(S):
        keep_in(2, s).start()
    read_all[z] = read_ref[...]
    for oz in range(1, Z):
        read_copy(oz, (z + Z - oz) % Z).wait_recv()
    for s in range(S):
        for kind in (1, 0):
            keep_in(kind, s).wait()
            give_in(kind, s, other).wait_recv()
        u_own[s] = state[s].astype(BF16)
    for _ in weight_steps(0):
        pass

    second = weight_steps(1)
    each(0, S, open_1)
    next(second, None)
    each(S, T, open_1)
    next(second, None)
    each(0, S, join_1)
    each(S, T, join_1)
    for _ in second:
        pass
    each(0, S, close_1)
    each(S, T, close_1)
    for s in range(S):
        give_in(2, s, a).start()
    each(0, T, join_2)
    each(0, T, close_2, 1.0)
    each(0, S, back_2)
    each(S, T, back_2)
    each(0, S, lambda s: exchange(0, [0, 1] + first_kinds, s))
    each(0, S, forward_1, True)
    each(S, T, forward_1, False)

    def step_end(s, step):
        moved = back_1(s, True)
        settle(s)
        fresh = state[s] - 0.005 * moved + 0.1 * noise[step, s]
        state[s] = fresh
        u_own[s] = fresh.astype(BF16)
        open_1(s)

    for s in range(S):
        keep_in(2, s).wait()
        give_in(2, s, other).wait_recv()
    each(0, S, step_end, 0)

    def data_end(s):
        back_1(S + s, False)
        settle(S + s)
        exchange(0, last_kinds, s)

    each(0, S, data_end)

    def langevin(step, carry):
        each(0, S, join_1)
        each(0, S, close_1)
        each(0, S, join_2)
        each(0, S, close_2, 1.0)
        each(0, S, back_2)
        each(0, S, forward_1, True)
        each(0, S, step_end, step)
        return carry

    lax.fori_loop(1, steps, langevin, 0)

    def contract(left, right):
        return lax.dot_general(
            left.reshape(-1, left.shape[-1]), right.reshape(-1, right.shape[-1]),
            (((0,), (0,)), ((), ())), preferred_element_type=F32,
        )

    each(0, S, lambda s: exchange(1, [0], s))
    each(0, S, join_1)
    each(0, S, close_1)
    each(0, S, lambda s: exchange(1, [1], s))
    each(0, S, join_2)
    arrived(0, range(2 + 2 * q))
    each(0, S, close_2, -1.0)
    for g, left, out_ref in ((1, rows_all, raw1_ref), (0, hid_all, raw2_ref)):
        for i in range(q):
            out_ref[:, i * C : (i + 1) * C] = contract(left[0], g_all[0, g, i])
    each(0, S, back_2)
    each(0, S, lambda s: exchange(1, first_kinds, s))
    each(0, S, forward_1, False)

    def last_end(s):
        back_1(s, False)
        exchange(1, last_kinds, s)

    each(0, S, last_end)

    squares = jnp.zeros((8, 128), F32)
    for g, left, out_ref in ((0, hid_all, raw2_ref), (1, rows_all, raw1_ref)):
        arrived(1, [1] + first_kinds if g == 0 else [0] + last_kinds)
        for i in range(q):
            at = slice(i * C, (i + 1) * C)
            raw = out_ref[:, at] + contract(left[1], g_all[1, g, i])
            out_ref[:, at] = raw
            squares += folded(raw * raw)
    own_stat[1] = squares
    gap = energy[S] - energy[0]
    for s in range(1, S):
        gap += energy[S + s] - energy[s]
    own_stat[0] = gap

    each(0, S, settle)
    for half in range(2):
        exchange_settle(half)
    for w in range(2):
        weight_settle(w)
    for oz in range(1, Z):
        read_copy(oz, z).wait_send()
    for kind in range(3):
        for s in range(S):
            give_in(kind, s, a).wait_send()

    base = 0
    for axis, count, peer in (("fsdp", X, x_peer), ("fsdp", Z, z_peer), ("dp", dpn, dp_peer)):
        copies = []
        for o in range(1, count):
            at = base + o - 1
            copy = send(own_stat, got_stat.at[at], sem_ts.at[at], sem_tr.at[at], {axis: peer(o)})
            copy.start()
            copies.append(copy)
        total = own_stat[...]
        for o, copy in enumerate(copies):
            copy.wait()
            total += got_stat[base + o]
        own_stat[...] = total
        base += count - 1
    stat_ref[...] = own_stat[...]


def solution(mesh):
    n, dpn = mesh.shape["fsdp"], mesh.shape["dp"]
    X = inner_of(n)
    Z = n // X
    K = Z // 2
    Y = dpn // 2
    q = n // dpn

    def local(data, start, noise, w1, w2, readout):
        R, C = start.shape
        H = w1.shape[1]
        steps = noise.shape[0]
        S = 2 if R % 64 == 0 else 1
        T = 2 * S
        h = R // T
        vmem = pl.BlockSpec(memory_space=pltpu.VMEM)
        hbm = pl.BlockSpec(memory_space=pl.ANY)
        dma = pltpu.SemaphoreType.DMA
        kinds = 2 + 2 * q
        others = 2 * dpn - 1
        peers = (X - 1) + (Z - 1) + (dpn - 1)
        wide = 2 * C
        X1, K1, Y1 = max(X - 1, 1), max(K - 1, 1), max(Y - 1, 1)
        raw1, raw2, stat = pl.pallas_call(
            functools.partial(kernel, n, X, dpn, steps, S),
            name="contrastive",
            out_shape=(
                jax.ShapeDtypeStruct((C, q * C), F32),
                jax.ShapeDtypeStruct((C, q * C), F32),
                jax.ShapeDtypeStruct((2, 8, 128), F32),
            ),
            in_specs=[hbm] * 5 + [vmem],
            out_specs=(vmem,) * 3,
            scratch_shapes=[
                pltpu.VMEM((wide, H), BF16),
                pltpu.VMEM((wide, H), BF16),
                pltpu.VMEM((S, h, wide), F32),
                pltpu.VMEM((steps, S, h, wide), F32),
                pltpu.VMEM((T, h, wide), BF16),
                pltpu.VMEM((T, h, wide), BF16),
                pltpu.VMEM((T, h, wide), F32),
                pltpu.VMEM((T, K, h, wide), F32),
                pltpu.VMEM((T, h, wide), F32),
                pltpu.VMEM((Z, 1, C), F32),
                pltpu.VMEM((T, 2, K, X1, h, wide), BF16),
                pltpu.VMEM((T, 2, K, X1, h, wide), BF16),
                pltpu.VMEM((T, 2 * K - 1, h, wide), BF16),
                pltpu.VMEM((T, K1, 1 + K, h, wide), BF16),
                pltpu.VMEM((T, 2, K * X, h, wide), BF16),
                pltpu.VMEM((2, 2 * dpn, S, h, C), BF16),
                pltpu.VMEM((2, 2 * dpn, S, h, C), BF16),
                pltpu.VMEM((2, 2, q, 2 * dpn, S, h, C), BF16),
                pltpu.VMEM((T, 8, 128), F32),
                pltpu.VMEM((2, 8, 128), F32),
                pltpu.VMEM((peers, 2, 8, 128), F32),
                dma((3 * S + 2,)),
                dma((3, S)), dma((3, S)),
                dma((Z - 1,)), dma((Z - 1,)),
                dma((2, PIECES)), dma((2, PIECES)),
                dma((2, PIECES, Y1)), dma((2, PIECES, Y1)),
                dma((2, PIECES, Y)), dma((2, PIECES, Y)),
                dma((T, 2, K, X1)), dma((T, 2, K, X1)),
                dma((T, K1, 1 + K)), dma((T, K1, 1 + K)),
                dma((T, K1)), dma((T, K1)),
                dma((T, 2, K, X1)), dma((T, 2, K, X1)),
                dma((2, kinds, others, S)), dma((2, kinds, others, S)),
                dma((peers,)), dma((peers,)),
            ],
            compiler_params=pltpu.CompilerParams(
                collective_id=0, has_side_effects=True, vmem_limit_bytes=60 * 1024 * 1024
            ),
        )(data, start, noise, w1, w2, readout.reshape(1, C))
        sums = jnp.sum(stat, axis=(1, 2))
        energy_gap = sums[0] / (R * dpn * 80.0 * jnp.sqrt(jnp.float32(H)))
        scale = jnp.sqrt(sums[1] / (2.0 * (C * n) * H) + 1e-06)
        return raw1 / scale, raw2 / scale, energy_gap

    in_specs = (
        P("dp", "fsdp"),
        P("dp", "fsdp"),
        P(None, "dp", "fsdp"),
        P("fsdp", None),
        P("fsdp", None),
        P("fsdp"),
    )
    out_specs = (P("fsdp", "dp"), P("fsdp", "dp"), P())
    return jax.shard_map(local, mesh=mesh, in_specs=in_specs, out_specs=out_specs, check_vma=False)
```

```python
import functools

import jax
import jax.numpy as jnp
from jax import lax
from jax.experimental import pallas as pl
from jax.experimental.pallas import tpu as pltpu
from jax.sharding import PartitionSpec as P

MESH = pl.DeviceIdType.MESH
BF16 = jnp.bfloat16
F32 = jnp.float32
PIECES = 4


def inner_of(n):
    return max(i for i in range(1, n + 1) if n % i == 0 and i * i <= n)


def folded(values):
    rows, columns = values.shape
    tall = values.reshape(rows // 8, 8, columns).sum(axis=0)
    out = tall[:, :128]
    for at in range(128, columns, 128):
        out += tall[:, at : at + 128]
    return out


def kernel(
    n, X, dpn, steps, S,
    data_ref, start_ref, noise_in, w1_ref, w2_ref, read_ref,
    raw1_ref, raw2_ref, stat_ref,
    wm1, wm2, u_in, start_in, s_u, r_u, acc_u, s_v, r_v,
    state, noise, u_own, hid, slope_1, acc, tot, read_all,
    s_a, r_a, s_b, r_b, buf, rows_all, hid_all, g_all, energy, own_stat, got_stat,
    sem_l, sem_us, sem_ur, sem_vs, sem_vr, sem_is, sem_ir, sem_ns, sem_nr, sem_rs, sem_rr, sem_wzs, sem_wzr, sem_wys, sem_wyr, sem_wcs, sem_wcr,
    sem_as, sem_ar, sem_bs, sem_br, sem_zs, sem_zr, sem_xs, sem_xr, sem_ds, sem_dr, sem_ts, sem_tr,
):
    Z = n // X
    K = Z // 2
    Y = dpn // 2
    T = 2 * S
    q = n // dpn
    C = w1_ref.shape[0]
    H = w1_ref.shape[1]
    h = state.shape[1]
    slice_rows = C // dpn
    piece = H // PIECES
    me = lax.axis_index("fsdp")
    dpi = lax.axis_index("dp")
    z, x = me // X, me % X
    k, a = z // 2, z % 2
    y, c = dpi // 2, dpi % 2
    other = 1 - a
    self_at = k * X + x

    def device(kd, ad, xd):
        return (kd * 2 + ad) * X + xd

    def x_peer(ox):
        return device(k, a, (x + ox) % X)

    def k_peer(ok):
        return device((k + ok) % K, a, x)

    def z_peer(oz):
        return ((z + oz) % Z) * X + x

    def dp_peer(o):
        return (dpi + o) % dpn

    def half_cols(at):
        return pl.ds(pl.multiple_of(at * C, C), C)

    def shard_cols(kd, i, xd):
        return pl.ds(pl.multiple_of(device(kd, i, xd) * C, C), C)

    def send(src, dst, ssem, rsem, peer):
        return pltpu.make_async_remote_copy(
            src_ref=src, dst_ref=dst, send_sem=ssem, recv_sem=rsem, device_id=peer, device_id_type=MESH
        )

    def fetch(src, dst, sem):
        return pltpu.make_async_copy(src, dst, sem)

    offsets = [(oa, od) for oa in range(2) for od in range(dpn) if (oa, od) != (0, 0)]

    def swap_peer(oa, od):
        return {"fsdp": device(k, (a + oa) % 2, x), "dp": dp_peer(od)}

    partners = (
        [{"fsdp": x_peer(ox)} for ox in range(1, X)]
        + [{"fsdp": z_peer(oz)} for oz in range(1, Z)]
        + [swap_peer(oa, od) for oa, od in offsets if od]
    )
    barrier = pltpu.get_barrier_semaphore()
    for peer in partners:
        pl.semaphore_signal(barrier, inc=1, device_id=peer, device_id_type=MESH)
    pl.semaphore_wait(barrier, len(partners))

    partner = {"fsdp": device(k, other, x)}

    def rows_in(half, s):
        return pl.ds(pl.multiple_of((half * S + s) * h, h), h)

    def fetch_in(g, ad, s):
        src, dst = ((start_ref, start_in.at[ad, s]), (data_ref, u_in.at[1, ad, s]))[g]
        return fetch(src.at[rows_in(ad, s), :], dst, sem_l.at[2 + (g * 2 + ad) * S + s])

    def give_state(s, slot):
        return send(
            start_in.at[other, s], state.at[s, :, half_cols(slot)], sem_is.at[s], sem_ir.at[s], partner
        )

    def keep_data(s):
        return fetch(
            data_ref.at[rows_in(a, s), :], u_own.at[S + s, :, half_cols(a)], sem_l.at[2 + 5 * S + s]
        )

    def give_data(s, slot):
        return send(
            u_in.at[1, other, s], u_own.at[S + s, :, half_cols(slot)], sem_is.at[S + s], sem_ir.at[S + s], partner
        )

    def keep_noise(s):
        return fetch(
            noise_in.at[:, rows_in(a, s), :], noise.at[:, s, :, half_cols(a)], sem_l.at[2 + 4 * S + s]
        )

    def give_noise(t, s, slot):
        return send(
            noise_in.at[t, rows_in(other, s), :], noise.at[t, s, :, half_cols(slot)],
            sem_ns.at[t, s], sem_nr.at[t, s], partner,
        )

    def read_copy(oz, at):
        return send(read_ref, read_all.at[at], sem_rs.at[oz - 1], sem_rr.at[oz - 1], {"fsdp": z_peer(oz)})

    weights = ((w1_ref, wm1), (w2_ref, wm2))

    def keep_w(w):
        src, dst = weights[w]
        return fetch(src, dst.at[half_cols(a), :], sem_l.at[w])

    def w_rows(slot, d):
        return pl.ds(pl.multiple_of(slot * C + d * slice_rows, slice_rows), slice_rows)

    def w_cols(p):
        return pl.ds(p * piece, piece)

    def wz_copy(w, p, slot):
        src, dst = weights[w]
        return send(
            src.at[w_rows(0, dpi), w_cols(p)], dst.at[w_rows(slot, dpi), w_cols(p)],
            sem_wzs.at[w, p], sem_wzr.at[w, p], partner,
        )

    def wy_copy(w, p, o, d):
        ref = weights[w][1].at[w_rows(other, d), w_cols(p)]
        return send(
            ref, ref, sem_wys.at[w, p, o - 1], sem_wyr.at[w, p, o - 1], {"dp": ((y + o) % Y) * 2 + c}
        )

    def wc_copy(w, p, o, d):
        ref = weights[w][1].at[w_rows(other, d), w_cols(p)]
        return send(ref, ref, sem_wcs.at[w, p, o], sem_wcr.at[w, p, o], {"dp": y * 2 + 1 - c})

    def y_source(o):
        return (y + Y - o) % Y

    def weight_steps(w):
        for p in range(PIECES + 1):
            if p < PIECES:
                wz_copy(w, p, other).wait_recv()
                for o in range(1, Y):
                    wy_copy(w, p, o, dpi).start()
                wc_copy(w, p, 0, dpi).start()
            if p:
                for o in range(1, Y):
                    d = y_source(o) * 2 + c
                    wy_copy(w, p - 1, o, d).wait_recv()
                    wc_copy(w, p - 1, o, d).start()
            yield
        for p in range(PIECES):
            for o in range(Y):
                wc_copy(w, p, o, y_source(o) * 2 + 1 - c).wait_recv()
        if w:
            keep_w(1).wait()

    def weight_settle(w):
        for p in range(PIECES):
            wz_copy(w, p, a).wait_send()
            for o in range(1, Y):
                wy_copy(w, p, o, dpi).wait_send()
            for o in range(Y):
                wc_copy(w, p, o, dpi).wait_send()

    order = list(range(1, K)) + [0]

    def ua_copy(g, ok, ox):
        return send(
            s_u.at[g, ok, ox - 1], r_u.at[g, ok, ox - 1], sem_us.at[g, ok, ox - 1], sem_ur.at[g, ok, ox - 1],
            {"fsdp": x_peer(ox)},
        )

    def ub_copy(g, ok, oa):
        ad = (a + oa) % 2
        return send(
            s_v.at[g, ok, ad], r_v.at[g, ok, oa], sem_vs.at[g, ok, oa], sem_vr.at[g, ok, oa],
            {"fsdp": device((k + ok) % K, ad, x)},
        )

    def first_open(g):
        lhs = u_in[g].reshape(T * h, C)
        for own in range(2):
            for ok in order:
                for ox in [0] if own else range(1, X):
                    for i in range(2):
                        cols = shard_cols((k + ok) % K, i, (x + ox) % X)
                        part = jnp.dot(lhs, wm1[half_cols(a), cols], preferred_element_type=F32)
                        if own:
                            acc_u[g, ok, :, i * C : (i + 1) * C] = part
                        else:
                            s_u[g, ok, ox - 1, :, i * C : (i + 1) * C] = part.astype(BF16)
                    if not own:
                        ua_copy(g, ok, ox).start()

    def first_join(g, ok):
        total = acc_u[g, ok]
        for ox in range(1, X):
            ua_copy(g, ok, ox).wait_recv()
            total += r_u[g, ok, ox - 1].astype(F32)
        s_v[g, ok] = total.astype(BF16).reshape(2, S * h, 2 * C)
        for oa in (0, 1):
            if ok or oa:
                ub_copy(g, ok, oa).start()
        if ok == 0:
            acc_u[g, 0] = total

    def first_close(g):
        a1 = acc_u[g, 0, pl.ds(pl.multiple_of(a * S * h, S * h), S * h), :]
        for ok in order:
            for oa in (0, 1):
                if ok or oa:
                    ub_copy(g, ok, oa).wait_recv()
                    a1 += r_v[g, ok, oa].astype(F32)
        s1 = jax.nn.sigmoid(a1)
        hidden = (a1 * s1).astype(BF16)
        slope = s1 * (1.0 + a1 * (1.0 - s1))
        for s in range(S):
            hid[g * S + s] = hidden[s * h : (s + 1) * h]
            slope_1[g * S + s] = slope[s * h : (s + 1) * h]

    def first_settle():
        for g in range(1):
            for ok in range(K):
                for ox in range(1, X):
                    ua_copy(g, ok, ox).wait_send()
                for oa in (0, 1):
                    if ok or oa:
                        ub_copy(g, ok, oa).wait_send()

    def a_copy(s, j, ok, ox):
        return send(
            s_a.at[s, j, ok, ox - 1], r_a.at[s, j, ok, ox - 1],
            sem_as.at[s, j, ok, ox - 1], sem_ar.at[s, j, ok, ox - 1], {"fsdp": x_peer(ox)},
        )

    def b_copy(s, j, ok, part):
        at = 0 if j == 0 else 1 + part
        return send(
            s_b.at[s, ok - 1 if j == 0 else K - 1 + part], r_b.at[s, ok - 1, at],
            sem_bs.at[s, ok - 1, at], sem_br.at[s, ok - 1, at], {"fsdp": k_peer(ok)},
        )

    def two_dots(lhs, w, kd, xd):
        return [
            jnp.dot(lhs, w[:, shard_cols(kd, i, xd)], preferred_element_type=F32) for i in range(2)
        ]

    def scatter_open(s, j, lhs, w):
        for ok in order:
            for ox in range(1, X):
                for i, part in enumerate(two_dots(lhs, w, (k + ok) % K, (x + ox) % X)):
                    s_a[s, j, ok, ox - 1, :, i * C : (i + 1) * C] = part.astype(BF16)
                a_copy(s, j, ok, ox).start()

    def pair(ref, low):
        return ref[pl.ds(low, S)].reshape(S * h, 2 * C)

    def pair_open(low, j, lhs, w):
        for ok in order:
            for ox in range(1, X):
                for i, part in enumerate(two_dots(lhs, w, (k + ok) % K, (x + ox) % X)):
                    for s in range(S):
                        s_a[low + s, j, ok, ox - 1, :, i * C : (i + 1) * C] = part[s * h : (s + 1) * h].astype(BF16)
                for s in range(S):
                    a_copy(low + s, j, ok, ox).start()

    def pair_own(low, lhs, w):
        for ok in order:
            for i, part in enumerate(two_dots(lhs, w, (k + ok) % K, x)):
                for s in range(S):
                    acc[low + s, ok, :, i * C : (i + 1) * C] = part[s * h : (s + 1) * h]

    def own_1(low):
        pair_own(low, pair(u_own, low), wm1)

    def own_2(low):
        pair_own(low, pair(hid, low), wm2)

    def pair_block(low, stage, kd, xd, w):
        total = None
        for i in range(2):
            lhs = buf[pl.ds(low, S), stage, kd * X + xd, :, i * C : (i + 1) * C].reshape(S * h, C)
            part = lax.dot_general(
                lhs, w[:, shard_cols(kd, i, xd)], (((1,), (1,)), ((), ())), preferred_element_type=F32
            )
            total = part if total is None else total + part
        return total

    def joined(s, j, ok):
        total = acc[s, ok]
        for ox in range(1, X):
            a_copy(s, j, ok, ox).wait_recv()
            total += r_a[s, j, ok, ox - 1].astype(F32)
        return total

    def open_1(s):
        scatter_open(s, 0, u_own[s], wm1)

    def join_1(s):
        for ok in range(1, K):
            s_b[s, ok - 1] = joined(s, 0, ok).astype(BF16)
            b_copy(s, 0, ok, 0).start()

    def hidden_1(s):
        a1 = joined(s, 0, 0)
        for ok in range(1, K):
            b_copy(s, 0, ok, 0).wait_recv()
            a1 += r_b[s, ok - 1, 0].astype(F32)
        s1 = jax.nn.sigmoid(a1)
        hid[s] = (a1 * s1).astype(BF16)
        slope_1[s] = s1 * (1.0 + a1 * (1.0 - s1))

    def close_1(s):
        hidden_1(s)
        scatter_open(s, 1, hid[s], wm2)

    def join_2(s):
        for ok in order:
            total = joined(s, 1, ok)
            acc[s, ok] = total
            s_b[s, K - 1 + ok] = total.astype(BF16)
            for to in range(1, K):
                b_copy(s, 1, to, ok).start()

    def x_copy(s, stage, ok, ox, at):
        ref = buf.at[s, stage, at]
        return send(
            ref, ref, sem_xs.at[s, stage, ok, ox - 1], sem_xr.at[s, stage, ok, ox - 1], {"fsdp": x_peer(ox)}
        )

    def z_copy(s, ok, at):
        ref = buf.at[s, 1, at]
        return send(ref, ref, sem_zs.at[s, ok - 1], sem_zr.at[s, ok - 1], {"fsdp": k_peer(ok)})

    def block(s, stage, kd, xd, w):
        total = None
        for i in range(2):
            part = lax.dot_general(
                buf[s, stage, kd * X + xd, :, i * C : (i + 1) * C], w[:, shard_cols(kd, i, xd)],
                (((1,), (1,)), ((), ())), preferred_element_type=F32,
            )
            total = part if total is None else total + part
        return total

    def close_2(s, sign):
        for ok in order:
            kd = (k + ok) % K
            a2 = acc[s, ok]
            for frm in range(1, K):
                part = (ok + frm) % K
                b_copy(s, 1, frm, part).wait_recv()
                a2 += r_b[s, frm - 1, 1 + part].astype(F32)
            gain = jnp.concatenate([read_all[kd * 2], read_all[kd * 2 + 1]], axis=1)
            s2 = jax.nn.sigmoid(a2)
            buf[s, 0, kd * X + x] = (sign * gain * (s2 * (1.0 + a2 * (1.0 - s2)))).astype(BF16)
            for ox in range(1, X):
                x_copy(s, 0, ok, ox, kd * X + x).start()
            if ok == 0:
                energy[s] = folded(gain * (a2 * s2))

    def mid_2(low):
        total = None
        for ok in order:
            part = pair_block(low, 0, (k + ok) % K, x, wm2)
            total = part if total is None else total + part
        tot[pl.ds(low, S)] = total.reshape(S, h, 2 * C)

    def back_2(s):
        total = tot[s]
        for ok in order:
            for ox in range(1, X):
                kd, xd = (k + ok) % K, (x + X - ox) % X
                x_copy(s, 0, ok, ox, kd * X + xd).wait_recv()
                total += block(s, 0, kd, xd, wm2)
        give_1(s, total)

    def give_1(s, total):
        buf[s, 1, self_at] = (total * slope_1[s]).astype(BF16)
        for ok in range(1, K):
            z_copy(s, ok, self_at).start()
        for ox in range(1, X):
            x_copy(s, 1, 0, ox, self_at).start()

    def pair_back_2(low):
        total = tot[pl.ds(low, S)].reshape(S * h, 2 * C)
        for ok in order:
            for ox in range(1, X):
                kd, xd = (k + ok) % K, (x + X - ox) % X
                for s in range(S):
                    x_copy(low + s, 0, ok, ox, kd * X + xd).wait_recv()
                total += pair_block(low, 0, kd, xd, wm2)
        for s in range(S):
            give_1(low + s, total[s * h : (s + 1) * h])

    def mid_1():
        tot[0:S] = pair_block(0, 1, k, x, wm1).reshape(S, h, 2 * C)

    def forward_1(s):
        for ok in range(1, K):
            kd = (k + K - ok) % K
            z_copy(s, ok, kd * X + x).wait_recv()
            for ox in range(1, X):
                x_copy(s, 1, ok, ox, kd * X + x).start()

    def more_1():
        total = tot[0:S].reshape(S * h, 2 * C)
        for ok in range(1, K):
            total += pair_block(0, 1, (k + K - ok) % K, x, wm1)
        for ox in range(1, X):
            xd = (x + X - ox) % X
            for s in range(S):
                x_copy(s, 1, 0, ox, k * X + xd).wait_recv()
            total += pair_block(0, 1, k, xd, wm1)
        tot[0:S] = total.reshape(S, h, 2 * C)

    def back_1(s, moving):
        if moving:
            total = tot[s]
        for ok in range(1, K) if moving else range(K):
            for ox in range(1, X):
                kd, xd = (k + K - ok) % K, (x + X - ox) % X
                x_copy(s, 1, ok, ox, kd * X + xd).wait_recv()
                if moving:
                    total += block(s, 1, kd, xd, wm1)
        if moving:
            return total

    def settle(s, first=False):
        for j in range(2):
            for ok in range(K):
                for ox in range(1, X):
                    if j or not first:
                        a_copy(s, j, ok, ox).wait_send()
                    x_copy(s, j, ok, ox, self_at).wait_send()
        for ok in range(1, K):
            if not first:
                b_copy(s, 0, ok, 0).wait_send()
            for part in range(K):
                b_copy(s, 1, ok, part).wait_send()
            z_copy(s, ok, self_at).wait_send()

    def place(half, kind, d, ad, s):
        if kind == 0:
            return rows_all.at[half, d, ad, s]
        if kind == 1:
            return hid_all.at[half, d, ad, s]
        return g_all.at[half, (kind - 2) // q, (kind - 2) % q, d, ad, s]

    def source(half, kind, s, ad, dd):
        at = s if half else S + s
        if kind == 0:
            return u_own.at[at, :, half_cols(ad)]
        if kind == 1:
            return hid.at[at, :, half_cols(ad)]
        stage, i = (kind - 2) // q, (kind - 2) % q
        shard = dd * q + i
        zd, xd = shard // X, shard % X
        return buf.at[at, stage, (zd // 2) * X + xd, :, half_cols(zd % 2)]

    def swap(half, kind, e, s, d, ad):
        oa, od = offsets[e]
        return send(
            source(half, kind, s, (a + oa) % 2, dp_peer(od)), place(half, kind, d, ad, s),
            sem_ds.at[half, kind, e, s], sem_dr.at[half, kind, e, s], swap_peer(oa, od),
        )

    def rows_copy(o, d):
        return send(
            u_in.at[1], rows_all.at[0, d], sem_ds.at[0, 0, o - 1, 0], sem_dr.at[0, 0, o - 1, 0], {"dp": dp_peer(o)}
        )

    def exchange_part(half, kinds, s, part):
        for kind in kinds:
            for e, (oa, _) in enumerate(offsets):
                if oa == part:
                    swap(half, kind, e, s, dpi, a).start()

    def exchange_near(half, kinds, s):
        exchange_part(half, kinds, s, 0)
        for kind in kinds:
            place(half, kind, dpi, a, s)[...] = source(half, kind, s, a, dpi)[...]

    def exchange_far(half, kinds, s):
        exchange_part(half, kinds, s, 1)

    def arrived(half, kinds):
        def one(s):
            for kind in kinds:
                for e, (oa, od) in enumerate(offsets):
                    swap(half, kind, e, s, (dpi + dpn - od) % dpn, (a + oa) % 2).wait_recv()

        each(0, S, one)

    data_kinds = range(1, 2 + 2 * q)

    def exchange_settle(half):
        def one(s):
            for kind in range(2 + 2 * q) if half else data_kinds:
                for e in range(len(offsets)):
                    swap(half, kind, e, s, dpi, a).wait_send()

        each(0, S, one)

    def each(low, high, stage, *args):
        def body(s, carry):
            stage(s, *args)
            return carry

        lax.fori_loop(low, high, body, 0)

    first_kinds, last_kinds = [2 + i for i in range(q)], [2 + q + i for i in range(q)]

    for p in range(PIECES):
        wz_copy(1, p, a).start()
    for s in range(S):
        for ad in range(2):
            fetch_in(0, ad, s).start()
    keep_w(0).start()
    for s in range(S):
        for ad in range(2):
            fetch_in(1, ad, s).start()
    keep_w(1).start()
    for s in range(S):
        keep_data(s).start()
        keep_noise(s).start()
    for oz in range(1, Z):
        read_copy(oz, z).start()
    for s in range(S):
        for ad in range(2):
            fetch_in(0, ad, s).wait()
    u_in[0] = start_in[...].astype(BF16)
    keep_w(0).wait()
    first_open(0)
    read_all[z] = read_ref[...]
    for s in range(S):
        state[s, :, half_cols(a)] = start_in[a, s]
    def step_end(s, step, first=False):
        moved = back_1(s, True)
        settle(s, first)
        give_noise(step, s, other).wait_recv()
        fresh = state[s] - 0.005 * moved + 0.1 * noise[step, s]
        state[s] = fresh
        u_own[s] = fresh.astype(BF16)
        open_1(s)

    for s in range(S):
        for ad in range(2):
            fetch_in(1, ad, s).wait()
    second, first = weight_steps(1), weight_steps(0)
    for ok in order:
        next(second)
        first_join(0, ok)
    for p in range(PIECES // 2):
        wz_copy(0, p, a).start()
    for _ in second:
        pass
    for oz in range(1, Z):
        read_copy(oz, (z + Z - oz) % Z).wait_recv()
    first_close(0)
    pair_open(0, 1, pair(hid, 0), wm2)
    own_2(0)
    next(first)
    each(0, S, join_2)
    for p in range(PIECES // 2, PIECES):
        wz_copy(0, p, a).start()
    for s in range(S):
        give_state(s, a).start()
        give_noise(0, s, a).start()
    next(first)
    each(0, S, close_2, 1.0)
    mid_2(0)
    next(first)
    each(0, S, back_2)
    for s in range(S):
        give_data(s, a).start()
    for _ in first:
        pass
    mid_1()
    each(0, S, forward_1)
    more_1()
    if steps > 1:
        for s in range(S):
            give_noise(1, s, a).start()
    for o in range(1, dpn):
        rows_copy(o, dpi).start()
    rows_all[0, dpi] = u_in[1]

    for s in range(S):
        keep_noise(s).wait()
        give_state(s, other).wait_recv()
    each(0, S, step_end, 0, True)
    own_1(0)

    def swap_task(kind, s):
        def task():
            exchange_near(0, [kind], s)
            exchange_far(0, [kind], s)

        return task

    def data_open():
        for s in range(S):
            keep_data(s).wait()
            give_data(s, other).wait_recv()
        pair_open(S, 0, pair(u_own, S), wm1)
        own_1(S)

    def data_middle():
        each(S, T, hidden_1)
        pair_open(S, 1, pair(hid, S), wm2)
        own_2(S)

    def data_close():
        each(S, T, close_2, 1.0)

    def data_back():
        mid_2(S)
        pair_back_2(S)

    def data_last():
        def last(s):
            back_1(s, False)
            settle(s)

        each(S, T, last)

    heavy = [
        data_open, lambda: each(S, T, join_1), data_middle, lambda: each(S, T, join_2), data_close,
        data_back, lambda: each(S, T, forward_1), data_last,
    ]
    light = [[] for _ in range(4 * max(steps - 1, 0))]
    late = []
    ready = {3: [1], 6: first_kinds, 8: last_kinds}
    at = 0
    for begin, kinds in ready.items():
        at = max(at, begin)
        for kind in kinds:
            for s in range(S):
                (light[at] if at < len(light) else late).append(swap_task(kind, s))
                at += s % 2 if kind > 1 + q else 1

    def slot(step, i):
        for t in range(1, steps):
            at = (t - 1) * 4 + i
            tasks = heavy[at : at + 1] + light[at]
            if tasks:

                @pl.when(step == t)
                def _(tasks=tasks):
                    for task in tasks:
                        task()

    def langevin(step, carry):
        each(0, S, join_1)
        slot(step, 0)
        each(0, S, close_1)
        own_2(0)
        each(0, S, join_2)
        slot(step, 1)
        each(0, S, close_2, 1.0)
        mid_2(0)
        each(0, S, back_2)
        slot(step, 2)
        mid_1()
        each(0, S, forward_1)
        more_1()

        @pl.when(step + 1 < steps)
        def _():
            for s in range(S):
                give_noise(step + 1, s, a).start()

        slot(step, 3)
        each(0, S, step_end, step)
        own_1(0)
        return carry

    lax.fori_loop(1, steps, langevin, 0)
    for task in heavy[4 * max(steps - 1, 0) :] + late:
        task()

    def contract(left, right):
        return lax.dot_general(
            left.reshape(-1, left.shape[-1]), right.reshape(-1, right.shape[-1]),
            (((0,), (0,)), ((), ())), preferred_element_type=F32,
        )

    for part in (exchange_near, exchange_far):
        each(0, S, lambda s: part(1, [0], s))
    each(0, S, join_1)
    each(0, S, close_1)
    own_2(0)
    for part in (exchange_near, exchange_far):
        each(0, S, lambda s: part(1, [1], s))
    each(0, S, join_2)
    each(0, S, close_2, -1.0)
    mid_2(0)
    each(0, S, back_2)
    each(0, S, lambda s: exchange_near(1, first_kinds, s))
    each(0, S, forward_1)
    each(0, S, lambda s: exchange_far(1, first_kinds, s))

    def last_end(s):
        back_1(s, False)
        exchange_near(1, last_kinds, s)
        exchange_far(1, last_kinds, s)

    each(0, S, last_end)

    for o in range(1, dpn):
        rows_copy(o, (dpi + dpn - o) % dpn).wait_recv()
    arrived(0, data_kinds)
    for g, left, out_ref in ((1, rows_all, raw1_ref), (0, hid_all, raw2_ref)):
        for i in range(q):
            out_ref[:, i * C : (i + 1) * C] = contract(left[0], g_all[0, g, i])

    squares = jnp.zeros((8, 128), F32)
    for g, left, out_ref in ((0, hid_all, raw2_ref), (1, rows_all, raw1_ref)):
        arrived(1, [1] + first_kinds if g == 0 else [0] + last_kinds)
        for i in range(q):
            at = slice(i * C, (i + 1) * C)
            raw = out_ref[:, at] + contract(left[1], g_all[1, g, i])
            out_ref[:, at] = raw
            squares += folded(raw * raw)
    own_stat[1] = squares
    gap = energy[S] - energy[0]
    for s in range(1, S):
        gap += energy[S + s] - energy[s]
    own_stat[0] = gap

    each(0, S, settle)
    for half in range(2):
        exchange_settle(half)
    for w in range(2):
        weight_settle(w)
    for oz in range(1, Z):
        read_copy(oz, z).wait_send()
    for s in range(S):
        give_state(s, a).wait_send()
        give_data(s, a).wait_send()
        for t in range(steps):
            give_noise(t, s, a).wait_send()
    for o in range(1, dpn):
        rows_copy(o, dpi).wait_send()
    first_settle()

    base = 0
    for axis, count, peer in (("fsdp", X, x_peer), ("fsdp", Z, z_peer), ("dp", dpn, dp_peer)):
        copies = []
        for o in range(1, count):
            at = base + o - 1
            copy = send(own_stat, got_stat.at[at], sem_ts.at[at], sem_tr.at[at], {axis: peer(o)})
            copy.start()
            copies.append(copy)
        total = own_stat[...]
        for o, copy in enumerate(copies):
            copy.wait()
            total += got_stat[base + o]
        own_stat[...] = total
        base += count - 1
    stat_ref[...] = own_stat[...]


def solution(mesh):
    n, dpn = mesh.shape["fsdp"], mesh.shape["dp"]
    X = inner_of(n)
    Z = n // X
    K = Z // 2
    Y = dpn // 2
    q = n // dpn

    def local(data, start, noise, w1, w2, readout):
        R, C = start.shape
        H = w1.shape[1]
        steps = noise.shape[0]
        S = 2 if R % 64 == 0 else 1
        T = 2 * S
        h = R // T
        vmem = pl.BlockSpec(memory_space=pltpu.VMEM)
        hbm = pl.BlockSpec(memory_space=pl.ANY)
        dma = pltpu.SemaphoreType.DMA
        kinds = 2 + 2 * q
        others = 2 * dpn - 1
        peers = (X - 1) + (Z - 1) + (dpn - 1)
        wide = 2 * C
        X1, K1, Y1 = max(X - 1, 1), max(K - 1, 1), max(Y - 1, 1)
        raw1, raw2, stat = pl.pallas_call(
            functools.partial(kernel, n, X, dpn, steps, S),
            name="contrastive",
            out_shape=(
                jax.ShapeDtypeStruct((C, q * C), F32),
                jax.ShapeDtypeStruct((C, q * C), F32),
                jax.ShapeDtypeStruct((2, 8, 128), F32),
            ),
            in_specs=[hbm] * 5 + [vmem],
            out_specs=(vmem,) * 3,
            scratch_shapes=[
                pltpu.VMEM((wide, H), BF16),
                pltpu.VMEM((wide, H), BF16),
                pltpu.VMEM((2, 2, S, h, C), BF16),
                pltpu.VMEM((2, S, h, C), F32),
                pltpu.VMEM((1, K, X1, R, wide), BF16),
                pltpu.VMEM((1, K, X1, R, wide), BF16),
                pltpu.VMEM((1, K, R, wide), F32),
                pltpu.VMEM((1, K, 2, S * h, wide), BF16),
                pltpu.VMEM((1, K, 2, S * h, wide), BF16),
                pltpu.VMEM((S, h, wide), F32),
                pltpu.VMEM((steps, S, h, wide), F32),
                pltpu.VMEM((T, h, wide), BF16),
                pltpu.VMEM((T, h, wide), BF16),
                pltpu.VMEM((T, h, wide), F32),
                pltpu.VMEM((T, K, h, wide), F32),
                pltpu.VMEM((T, h, wide), F32),
                pltpu.VMEM((Z, 1, C), F32),
                pltpu.VMEM((T, 2, K, X1, h, wide), BF16),
                pltpu.VMEM((T, 2, K, X1, h, wide), BF16),
                pltpu.VMEM((T, 2 * K - 1, h, wide), BF16),
                pltpu.VMEM((T, K1, 1 + K, h, wide), BF16),
                pltpu.VMEM((T, 2, K * X, h, wide), BF16),
                pltpu.VMEM((2, dpn, 2, S, h, C), BF16),
                pltpu.VMEM((2, dpn, 2, S, h, C), BF16),
                pltpu.VMEM((2, 2, q, dpn, 2, S, h, C), BF16),
                pltpu.VMEM((T, 8, 128), F32),
                pltpu.VMEM((2, 8, 128), F32),
                pltpu.VMEM((peers, 2, 8, 128), F32),
                dma((2 + 6 * S,)),
                dma((1, K, X1)), dma((1, K, X1)),
                dma((1, K, 2)), dma((1, K, 2)),
                dma((T,)), dma((T,)),
                dma((steps, S)), dma((steps, S)),
                dma((Z - 1,)), dma((Z - 1,)),
                dma((2, PIECES)), dma((2, PIECES)),
                dma((2, PIECES, Y1)), dma((2, PIECES, Y1)),
                dma((2, PIECES, Y)), dma((2, PIECES, Y)),
                dma((T, 2, K, X1)), dma((T, 2, K, X1)),
                dma((T, K1, 1 + K)), dma((T, K1, 1 + K)),
                dma((T, K1)), dma((T, K1)),
                dma((T, 2, K, X1)), dma((T, 2, K, X1)),
                dma((2, kinds, others, S)), dma((2, kinds, others, S)),
                dma((peers,)), dma((peers,)),
            ],
            compiler_params=pltpu.CompilerParams(
                collective_id=0, has_side_effects=True, vmem_limit_bytes=60 * 1024 * 1024
            ),
        )(data, start, noise, w1, w2, readout.reshape(1, C))
        sums = jnp.sum(stat, axis=(1, 2))
        energy_gap = sums[0] / (R * dpn * 80.0 * jnp.sqrt(jnp.float32(H)))
        scale = jnp.sqrt(sums[1] / (2.0 * (C * n) * H) + 1e-06)
        return raw1 / scale, raw2 / scale, energy_gap

    in_specs = (
        P("dp", "fsdp"),
        P("dp", "fsdp"),
        P(None, "dp", "fsdp"),
        P("fsdp", None),
        P("fsdp", None),
        P("fsdp"),
    )
    out_specs = (P("fsdp", "dp"), P("fsdp", "dp"), P())
    return jax.shard_map(local, mesh=mesh, in_specs=in_specs, out_specs=out_specs, check_vma=False)
```

```python
import functools

import jax
import jax.numpy as jnp
from jax import lax
from jax.experimental import pallas as pl
from jax.experimental.pallas import tpu as pltpu
from jax.sharding import PartitionSpec as P

MESH = pl.DeviceIdType.MESH
BF16 = jnp.bfloat16
F32 = jnp.float32
PIECES = 8
EARLY = 2
TASK_SLOTS = (0, 1, 2, 3, 4, 5, 6, 7)


def inner_of(n):
    return max(i for i in range(1, n + 1) if n % i == 0 and i * i <= n)


def folded(values):
    rows, columns = values.shape
    tall = values.reshape(rows // 8, 8, columns).sum(axis=0)
    out = tall[:, :128]
    for at in range(128, columns, 128):
        out += tall[:, at : at + 128]
    return out


def kernel(
    n, X, dpn, steps, S,
    data_ref, start_ref, noise_in, w1_ref, w2_ref, read_ref,
    raw1_out, raw2_out, stat_ref, raw1_ref, raw2_ref,
    wm1, wm2, u_in, start_in, s_u, r_u, acc_u, s_v, r_v,
    state, noise, u_own, hid, slope_1, acc, tot, read_all,
    s_a, r_a, s_b, r_b, buf, rows_all, hid_all, g_all, energy, own_stat, got_stat,
    sem_l, sem_us, sem_ur, sem_vs, sem_vr, sem_is, sem_ir, sem_ns, sem_nr, sem_rs, sem_rr, sem_wzs, sem_wzr, sem_wys, sem_wyr, sem_wcs, sem_wcr,
    sem_as, sem_ar, sem_bs, sem_br, sem_zs, sem_zr, sem_xs, sem_xr, sem_ds, sem_dr, sem_ts, sem_tr,
):
    Z = n // X
    K = Z // 2
    Y = dpn // 2
    T = 2 * S
    q = n // dpn
    C = w1_ref.shape[0]
    H = w1_ref.shape[1]
    h = state.shape[1]
    slice_rows = C // dpn
    piece = H // PIECES
    me = lax.axis_index("fsdp")
    dpi = lax.axis_index("dp")
    z, x = me // X, me % X
    k, a = z // 2, z % 2
    y, c = dpi // 2, dpi % 2
    other = 1 - a
    self_at = k * X + x

    def device(kd, ad, xd):
        return (kd * 2 + ad) * X + xd

    def x_peer(ox):
        return device(k, a, (x + ox) % X)

    def k_peer(ok):
        return device((k + ok) % K, a, x)

    def z_peer(oz):
        return ((z + oz) % Z) * X + x

    def dp_peer(o):
        return (dpi + o) % dpn

    def half_cols(at):
        return pl.ds(pl.multiple_of(at * C, C), C)

    def shard_cols(kd, i, xd):
        return pl.ds(pl.multiple_of(device(kd, i, xd) * C, C), C)

    def send(src, dst, ssem, rsem, peer):
        return pltpu.make_async_remote_copy(
            src_ref=src, dst_ref=dst, send_sem=ssem, recv_sem=rsem, device_id=peer, device_id_type=MESH
        )

    def fetch(src, dst, sem):
        return pltpu.make_async_copy(src, dst, sem)

    offsets = [(oa, od) for oa in range(2) for od in range(dpn) if (oa, od) != (0, 0)]

    def swap_peer(oa, od):
        return {"fsdp": device(k, (a + oa) % 2, x), "dp": dp_peer(od)}

    partners = (
        [{"fsdp": x_peer(ox)} for ox in range(1, X)]
        + [{"fsdp": z_peer(oz)} for oz in range(1, Z)]
        + [swap_peer(oa, od) for oa, od in offsets if od]
    )
    barrier = pltpu.get_barrier_semaphore()
    for peer in partners:
        pl.semaphore_signal(barrier, inc=1, device_id=peer, device_id_type=MESH)
    pl.semaphore_wait(barrier, len(partners))

    partner = {"fsdp": device(k, other, x)}

    def rows_in(half, s):
        return pl.ds(pl.multiple_of((half * S + s) * h, h), h)

    def fetch_in(g, ad, s):
        src, dst = ((start_ref, start_in.at[ad, s]), (data_ref, u_in.at[1, ad, s]))[g]
        return fetch(src.at[rows_in(ad, s), :], dst, sem_l.at[2 + (g * 2 + ad) * S + s])

    def give_state(s, slot):
        return send(
            start_in.at[other, s], state.at[s, :, half_cols(slot)], sem_is.at[s], sem_ir.at[s], partner
        )

    def keep_data(s):
        return fetch(
            data_ref.at[rows_in(a, s), :], u_own.at[S + s, :, half_cols(a)], sem_l.at[2 + 5 * S + s]
        )

    def give_data(s, slot):
        return send(
            u_in.at[1, other, s], u_own.at[S + s, :, half_cols(slot)], sem_is.at[S + s], sem_ir.at[S + s], partner
        )

    def keep_noise(s):
        return fetch(
            noise_in.at[:, rows_in(a, s), :], noise.at[:, s, :, half_cols(a)], sem_l.at[2 + 4 * S + s]
        )

    def give_noise(t, s, slot):
        return send(
            noise_in.at[t, rows_in(other, s), :], noise.at[t, s, :, half_cols(slot)],
            sem_ns.at[t, s], sem_nr.at[t, s], partner,
        )

    def read_copy(oz, at):
        return send(read_ref, read_all.at[at], sem_rs.at[oz - 1], sem_rr.at[oz - 1], {"fsdp": z_peer(oz)})

    weights = ((w1_ref, wm1), (w2_ref, wm2))

    def keep_w(w):
        src, dst = weights[w]
        return fetch(src, dst.at[half_cols(a), :], sem_l.at[w])

    def w_rows(slot, d):
        return pl.ds(pl.multiple_of(slot * C + d * slice_rows, slice_rows), slice_rows)

    def w_cols(p):
        return pl.ds(p * piece, piece)

    def wz_copy(w, p, slot):
        src, dst = weights[w]
        return send(
            src.at[w_rows(0, dpi), w_cols(p)], dst.at[w_rows(slot, dpi), w_cols(p)],
            sem_wzs.at[w, p], sem_wzr.at[w, p], partner,
        )

    def wy_copy(w, p, o, d):
        ref = weights[w][1].at[w_rows(other, d), w_cols(p)]
        return send(
            ref, ref, sem_wys.at[w, p, o - 1], sem_wyr.at[w, p, o - 1], {"dp": ((y + o) % Y) * 2 + c}
        )

    def wc_copy(w, p, o, d):
        ref = weights[w][1].at[w_rows(other, d), w_cols(p)]
        return send(ref, ref, sem_wcs.at[w, p, o], sem_wcr.at[w, p, o], {"dp": y * 2 + 1 - c})

    def y_source(o):
        return (y + Y - o) % Y

    def weight_steps(w):
        for p in range(PIECES + 1):
            if p < PIECES:
                wz_copy(w, p, other).wait_recv()
                for o in range(1, Y):
                    wy_copy(w, p, o, dpi).start()
                wc_copy(w, p, 0, dpi).start()
            if p:
                for o in range(1, Y):
                    d = y_source(o) * 2 + c
                    wy_copy(w, p - 1, o, d).wait_recv()
                    wc_copy(w, p - 1, o, d).start()
            yield
        for p in range(PIECES):
            for o in range(Y):
                wc_copy(w, p, o, y_source(o) * 2 + 1 - c).wait_recv()
        if w:
            keep_w(1).wait()

    def advance(steps_of):
        for _ in range(PIECES // 4):
            next(steps_of)

    def weight_settle(w):
        for p in range(PIECES):
            wz_copy(w, p, a).wait_send()
            for o in range(1, Y):
                wy_copy(w, p, o, dpi).wait_send()
            for o in range(Y):
                wc_copy(w, p, o, dpi).wait_send()

    order = list(range(1, K)) + [0]

    def ua_copy(g, ok, ox):
        return send(
            s_u.at[g, ok, ox - 1], r_u.at[g, ok, ox - 1], sem_us.at[g, ok, ox - 1], sem_ur.at[g, ok, ox - 1],
            {"fsdp": x_peer(ox)},
        )

    def ub_copy(g, ok, oa):
        ad = (a + oa) % 2
        return send(
            s_v.at[g, ok, ad], r_v.at[g, ok, oa], sem_vs.at[g, ok, oa], sem_vr.at[g, ok, oa],
            {"fsdp": device((k + ok) % K, ad, x)},
        )

    def first_open(g):
        lhs = u_in[g].reshape(T * h, C)
        for own in range(2):
            for ok in order:
                for ox in [0] if own else range(1, X):
                    for i in range(2):
                        cols = shard_cols((k + ok) % K, i, (x + ox) % X)
                        part = jnp.dot(lhs, wm1[half_cols(a), cols], preferred_element_type=F32)
                        if own:
                            acc_u[g, ok, :, i * C : (i + 1) * C] = part
                        else:
                            s_u[g, ok, ox - 1, :, i * C : (i + 1) * C] = part.astype(BF16)
                    if not own:
                        ua_copy(g, ok, ox).start()

    def first_join(g, ok):
        total = acc_u[g, ok]
        for ox in range(1, X):
            ua_copy(g, ok, ox).wait_recv()
            total += r_u[g, ok, ox - 1].astype(F32)
        s_v[g, ok] = total.astype(BF16).reshape(2, S * h, 2 * C)
        for oa in (0, 1):
            if ok or oa:
                ub_copy(g, ok, oa).start()
        if ok == 0:
            acc_u[g, 0] = total

    def first_close(g):
        a1 = acc_u[g, 0, pl.ds(pl.multiple_of(a * S * h, S * h), S * h), :]
        for ok in order:
            for oa in (0, 1):
                if ok or oa:
                    ub_copy(g, ok, oa).wait_recv()
                    a1 += r_v[g, ok, oa].astype(F32)
        s1 = jax.nn.sigmoid(a1)
        hidden = (a1 * s1).astype(BF16)
        slope = s1 * (1.0 + a1 * (1.0 - s1))
        for s in range(S):
            hid[g * S + s] = hidden[s * h : (s + 1) * h]
            slope_1[g * S + s] = slope[s * h : (s + 1) * h]

    def first_settle():
        for g in range(1):
            for ok in range(K):
                for ox in range(1, X):
                    ua_copy(g, ok, ox).wait_send()
                for oa in (0, 1):
                    if ok or oa:
                        ub_copy(g, ok, oa).wait_send()

    def a_copy(s, j, ok, ox):
        return send(
            s_a.at[s, j, ok, ox - 1], r_a.at[s, j, ok, ox - 1],
            sem_as.at[s, j, ok, ox - 1], sem_ar.at[s, j, ok, ox - 1], {"fsdp": x_peer(ox)},
        )

    def b_copy(s, j, ok, part):
        at = 0 if j == 0 else 1 + part
        return send(
            s_b.at[s, ok - 1 if j == 0 else K - 1 + part], r_b.at[s, ok - 1, at],
            sem_bs.at[s, ok - 1, at], sem_br.at[s, ok - 1, at], {"fsdp": k_peer(ok)},
        )

    def two_dots(lhs, w, kd, xd):
        return [
            jnp.dot(lhs, w[:, shard_cols(kd, i, xd)], preferred_element_type=F32) for i in range(2)
        ]

    def scatter_open(s, j, lhs, w):
        for ok in order:
            for ox in range(1, X):
                for i, part in enumerate(two_dots(lhs, w, (k + ok) % K, (x + ox) % X)):
                    s_a[s, j, ok, ox - 1, :, i * C : (i + 1) * C] = part.astype(BF16)
                a_copy(s, j, ok, ox).start()

    def pair(ref, low):
        return ref[pl.ds(low, S)].reshape(S * h, 2 * C)

    def pair_open(low, j, lhs, w):
        for ok in order:
            for ox in range(1, X):
                for i, part in enumerate(two_dots(lhs, w, (k + ok) % K, (x + ox) % X)):
                    for s in range(S):
                        s_a[low + s, j, ok, ox - 1, :, i * C : (i + 1) * C] = part[s * h : (s + 1) * h].astype(BF16)
                for s in range(S):
                    a_copy(low + s, j, ok, ox).start()

    def pair_own(low, lhs, w):
        for ok in order:
            for i, part in enumerate(two_dots(lhs, w, (k + ok) % K, x)):
                for s in range(S):
                    acc[low + s, ok, :, i * C : (i + 1) * C] = part[s * h : (s + 1) * h]

    def own_1(low):
        pair_own(low, pair(u_own, low), wm1)

    def own_2(low):
        pair_own(low, pair(hid, low), wm2)

    def pair_block(low, stage, kd, xd, w):
        total = None
        for i in range(2):
            lhs = buf[pl.ds(low, S), stage, kd * X + xd, :, i * C : (i + 1) * C].reshape(S * h, C)
            part = lax.dot_general(
                lhs, w[:, shard_cols(kd, i, xd)], (((1,), (1,)), ((), ())), preferred_element_type=F32
            )
            total = part if total is None else total + part
        return total

    def joined(s, j, ok):
        total = acc[s, ok]
        for ox in range(1, X):
            a_copy(s, j, ok, ox).wait_recv()
            total += r_a[s, j, ok, ox - 1].astype(F32)
        return total

    def open_1(s):
        scatter_open(s, 0, u_own[s], wm1)

    def join_1(s):
        for ok in range(1, K):
            s_b[s, ok - 1] = joined(s, 0, ok).astype(BF16)
            b_copy(s, 0, ok, 0).start()

    def hidden_1(s):
        a1 = joined(s, 0, 0)
        for ok in range(1, K):
            b_copy(s, 0, ok, 0).wait_recv()
            a1 += r_b[s, ok - 1, 0].astype(F32)
        s1 = jax.nn.sigmoid(a1)
        hid[s] = (a1 * s1).astype(BF16)
        slope_1[s] = s1 * (1.0 + a1 * (1.0 - s1))

    def close_1(s):
        hidden_1(s)
        scatter_open(s, 1, hid[s], wm2)

    def join_2(s):
        for ok in order:
            total = joined(s, 1, ok)
            acc[s, ok] = total
            s_b[s, K - 1 + ok] = total.astype(BF16)
            for to in range(1, K):
                b_copy(s, 1, to, ok).start()

    def x_copy(s, stage, ok, ox, at):
        ref = buf.at[s, stage, at]
        return send(
            ref, ref, sem_xs.at[s, stage, ok, ox - 1], sem_xr.at[s, stage, ok, ox - 1], {"fsdp": x_peer(ox)}
        )

    def z_copy(s, ok, at):
        ref = buf.at[s, 1, at]
        return send(ref, ref, sem_zs.at[s, ok - 1], sem_zr.at[s, ok - 1], {"fsdp": k_peer(ok)})

    def block(s, stage, kd, xd, w):
        total = None
        for i in range(2):
            part = lax.dot_general(
                buf[s, stage, kd * X + xd, :, i * C : (i + 1) * C], w[:, shard_cols(kd, i, xd)],
                (((1,), (1,)), ((), ())), preferred_element_type=F32,
            )
            total = part if total is None else total + part
        return total

    def close_2(s, sign):
        for ok in order:
            kd = (k + ok) % K
            a2 = acc[s, ok]
            for frm in range(1, K):
                part = (ok + frm) % K
                b_copy(s, 1, frm, part).wait_recv()
                a2 += r_b[s, frm - 1, 1 + part].astype(F32)
            gain = jnp.concatenate([read_all[kd * 2], read_all[kd * 2 + 1]], axis=1)
            s2 = jax.nn.sigmoid(a2)
            buf[s, 0, kd * X + x] = (sign * gain * (s2 * (1.0 + a2 * (1.0 - s2)))).astype(BF16)
            for ox in range(1, X):
                x_copy(s, 0, ok, ox, kd * X + x).start()
            if ok == 0:
                energy[s] = folded(gain * (a2 * s2))

    def mid_2(low):
        total = None
        for ok in order:
            part = pair_block(low, 0, (k + ok) % K, x, wm2)
            total = part if total is None else total + part
        tot[pl.ds(low, S)] = total.reshape(S, h, 2 * C)

    def back_2(s):
        total = tot[s]
        for ok in order:
            for ox in range(1, X):
                kd, xd = (k + ok) % K, (x + X - ox) % X
                x_copy(s, 0, ok, ox, kd * X + xd).wait_recv()
                total += block(s, 0, kd, xd, wm2)
        give_1(s, total)

    def give_1(s, total):
        buf[s, 1, self_at] = (total * slope_1[s]).astype(BF16)
        for ok in range(1, K):
            z_copy(s, ok, self_at).start()
        for ox in range(1, X):
            x_copy(s, 1, 0, ox, self_at).start()

    def pair_back_2(low):
        total = tot[pl.ds(low, S)].reshape(S * h, 2 * C)
        for ok in order:
            for ox in range(1, X):
                kd, xd = (k + ok) % K, (x + X - ox) % X
                for s in range(S):
                    x_copy(low + s, 0, ok, ox, kd * X + xd).wait_recv()
                total += pair_block(low, 0, kd, xd, wm2)
        for s in range(S):
            give_1(low + s, total[s * h : (s + 1) * h])

    def mid_1():
        tot[0:S] = pair_block(0, 1, k, x, wm1).reshape(S, h, 2 * C)

    def forward_1(s):
        for ok in range(1, K):
            kd = (k + K - ok) % K
            z_copy(s, ok, kd * X + x).wait_recv()
            for ox in range(1, X):
                x_copy(s, 1, ok, ox, kd * X + x).start()

    def more_1():
        total = tot[0:S].reshape(S * h, 2 * C)
        for ok in range(1, K):
            total += pair_block(0, 1, (k + K - ok) % K, x, wm1)
        for ox in range(1, X):
            xd = (x + X - ox) % X
            for s in range(S):
                x_copy(s, 1, 0, ox, k * X + xd).wait_recv()
            total += pair_block(0, 1, k, xd, wm1)
        tot[0:S] = total.reshape(S, h, 2 * C)

    def back_1(s, moving):
        if moving:
            total = tot[s]
        for ok in range(1, K) if moving else range(K):
            for ox in range(1, X):
                kd, xd = (k + K - ok) % K, (x + X - ox) % X
                x_copy(s, 1, ok, ox, kd * X + xd).wait_recv()
                if moving:
                    total += block(s, 1, kd, xd, wm1)
        if moving:
            return total

    def settle(s, first=False):
        for j in range(2):
            for ok in range(K):
                for ox in range(1, X):
                    if j or not first:
                        a_copy(s, j, ok, ox).wait_send()
                    x_copy(s, j, ok, ox, self_at).wait_send()
        for ok in range(1, K):
            if not first:
                b_copy(s, 0, ok, 0).wait_send()
            for part in range(K):
                b_copy(s, 1, ok, part).wait_send()
            z_copy(s, ok, self_at).wait_send()

    def place(half, kind, d, ad, s):
        if kind == 0:
            return rows_all.at[half, d, ad, s]
        if kind == 1:
            return hid_all.at[half, d, ad, s]
        return g_all.at[half, (kind - 2) // q, (kind - 2) % q, d, ad, s]

    def source(half, kind, s, ad, dd):
        at = s if half else S + s
        if kind == 0:
            return u_own.at[at, :, half_cols(ad)]
        if kind == 1:
            return hid.at[at, :, half_cols(ad)]
        stage, i = (kind - 2) // q, (kind - 2) % q
        shard = dd * q + i
        zd, xd = shard // X, shard % X
        return buf.at[at, stage, (zd // 2) * X + xd, :, half_cols(zd % 2)]

    def swap(half, kind, e, s, d, ad):
        oa, od = offsets[e]
        return send(
            source(half, kind, s, (a + oa) % 2, dp_peer(od)), place(half, kind, d, ad, s),
            sem_ds.at[half, kind, e, s], sem_dr.at[half, kind, e, s], swap_peer(oa, od),
        )

    def rows_copy(o, d):
        return send(
            u_in.at[1], rows_all.at[0, d], sem_ds.at[0, 0, o - 1, 0], sem_dr.at[0, 0, o - 1, 0], {"dp": dp_peer(o)}
        )

    def exchange_part(half, kinds, s, part):
        for kind in kinds:
            for e, (oa, _) in enumerate(offsets):
                if oa == part:
                    swap(half, kind, e, s, dpi, a).start()

    def exchange_near(half, kinds, s):
        exchange_part(half, kinds, s, 0)
        for kind in kinds:
            place(half, kind, dpi, a, s)[...] = source(half, kind, s, a, dpi)[...]

    def exchange_far(half, kinds, s):
        exchange_part(half, kinds, s, 1)

    def arrived(half, kinds):
        def one(s):
            for kind in kinds:
                for e, (oa, od) in enumerate(offsets):
                    swap(half, kind, e, s, (dpi + dpn - od) % dpn, (a + oa) % 2).wait_recv()

        each(0, S, one)

    data_kinds = range(1, 2 + 2 * q)

    def exchange_settle(half):
        def one(s):
            for kind in range(2 + 2 * q) if half else data_kinds:
                for e in range(len(offsets)):
                    swap(half, kind, e, s, dpi, a).wait_send()

        each(0, S, one)

    def each(low, high, stage, *args):
        def body(s, carry):
            stage(s, *args)
            return carry

        lax.fori_loop(low, high, body, 0)

    first_kinds, last_kinds = [2 + i for i in range(q)], [2 + q + i for i in range(q)]

    for p in range(PIECES):
        wz_copy(1, p, a).start()
    for s in range(S):
        for ad in range(2):
            fetch_in(0, ad, s).start()
    keep_w(0).start()
    for s in range(S):
        for ad in range(2):
            fetch_in(1, ad, s).start()
    keep_w(1).start()
    for s in range(S):
        keep_data(s).start()
        keep_noise(s).start()
    for oz in range(1, Z):
        read_copy(oz, z).start()
    for s in range(S):
        for ad in range(2):
            fetch_in(0, ad, s).wait()
    u_in[0] = start_in[...].astype(BF16)
    keep_w(0).wait()
    first_open(0)
    read_all[z] = read_ref[...]
    for s in range(S):
        state[s, :, half_cols(a)] = start_in[a, s]
    def step_end(s, step, first=False):
        moved = back_1(s, True)
        settle(s, first)
        give_noise(step, s, other).wait_recv()
        fresh = state[s] - 0.005 * moved + 0.1 * noise[step, s]
        state[s] = fresh
        u_own[s] = fresh.astype(BF16)
        open_1(s)

    for s in range(S):
        for ad in range(2):
            fetch_in(1, ad, s).wait()
    second, first = weight_steps(1), weight_steps(0)
    for ok in order:
        advance(second)
        first_join(0, ok)
    for p in range(PIECES * EARLY // 4):
        wz_copy(0, p, a).start()
    for _ in second:
        pass
    for oz in range(1, Z):
        read_copy(oz, (z + Z - oz) % Z).wait_recv()
    first_close(0)
    pair_open(0, 1, pair(hid, 0), wm2)
    own_2(0)
    advance(first)
    each(0, S, join_2)
    for p in range(PIECES * EARLY // 4, PIECES):
        wz_copy(0, p, a).start()
    for s in range(S):
        give_state(s, a).start()
        give_noise(0, s, a).start()
    advance(first)
    each(0, S, close_2, 1.0)
    mid_2(0)
    advance(first)
    each(0, S, back_2)
    for s in range(S):
        give_data(s, a).start()
    for _ in first:
        pass
    mid_1()
    each(0, S, forward_1)
    more_1()
    if steps > 1:
        for s in range(S):
            give_noise(1, s, a).start()
    for o in range(1, dpn):
        rows_copy(o, dpi).start()
    rows_all[0, dpi] = u_in[1]

    for s in range(S):
        keep_noise(s).wait()
        give_state(s, other).wait_recv()
    each(0, S, step_end, 0, True)
    own_1(0)

    def swap_task(kind, s):
        def task():
            exchange_near(0, [kind], s)
            exchange_far(0, [kind], s)

        return task

    def data_open():
        for s in range(S):
            keep_data(s).wait()
            give_data(s, other).wait_recv()
        pair_open(S, 0, pair(u_own, S), wm1)
        own_1(S)

    def data_middle():
        each(S, T, hidden_1)
        pair_open(S, 1, pair(hid, S), wm2)
        own_2(S)

    def data_close():
        each(S, T, close_2, 1.0)

    def data_back():
        mid_2(S)
        pair_back_2(S)

    def data_last():
        def last(s):
            back_1(s, False)
            settle(s)

        each(S, T, last)

    heavy = [
        data_open, lambda: each(S, T, join_1), data_middle, lambda: each(S, T, join_2), data_close,
        data_back, lambda: each(S, T, forward_1), data_last,
    ]
    places = 4 * max(steps - 1, 0)
    duty = {at: task for at, task in zip(TASK_SLOTS, heavy)}
    light = [[] for _ in range(places)]
    late = []
    ready = {TASK_SLOTS[2] + 1: [1], TASK_SLOTS[5] + 1: first_kinds, TASK_SLOTS[7] + 1: last_kinds}
    at = 0
    for begin, kinds in ready.items():
        at = max(at, begin)
        for kind in kinds:
            for s in range(S):
                (light[at] if at < len(light) else late).append(swap_task(kind, s))
                at += s % 2 if kind > 1 + q else 1

    def slot(step, i):
        for t in range(1, steps):
            at = (t - 1) * 4 + i
            tasks = ([duty[at]] if at in duty else []) + light[at]
            if tasks:

                @pl.when(step == t)
                def _(tasks=tasks):
                    for task in tasks:
                        task()

    def langevin(step, carry):
        each(0, S, join_1)
        slot(step, 0)
        each(0, S, close_1)
        own_2(0)
        each(0, S, join_2)
        slot(step, 1)
        each(0, S, close_2, 1.0)
        mid_2(0)
        each(0, S, back_2)
        slot(step, 2)
        mid_1()
        each(0, S, forward_1)
        more_1()

        @pl.when(step + 1 < steps)
        def _():
            for s in range(S):
                give_noise(step + 1, s, a).start()

        slot(step, 3)
        each(0, S, step_end, step)
        own_1(0)
        return carry

    lax.fori_loop(1, steps, langevin, 0)
    for task in [duty[at] for at in TASK_SLOTS if at >= places] + late:
        task()

    def contract(left, right):
        return lax.dot_general(
            left.reshape(-1, left.shape[-1]), right.reshape(-1, right.shape[-1]),
            (((0,), (0,)), ((), ())), preferred_element_type=F32,
        )

    for part in (exchange_near, exchange_far):
        each(0, S, lambda s: part(1, [0], s))
    each(0, S, join_1)
    each(0, S, close_1)
    own_2(0)
    for part in (exchange_near, exchange_far):
        each(0, S, lambda s: part(1, [1], s))
    each(0, S, join_2)
    each(0, S, close_2, -1.0)
    mid_2(0)
    each(0, S, back_2)
    each(0, S, lambda s: exchange_near(1, first_kinds, s))
    each(0, S, forward_1)
    each(0, S, lambda s: exchange_far(1, first_kinds, s))

    def last_end(s):
        back_1(s, False)
        exchange_near(1, last_kinds, s)
        exchange_far(1, last_kinds, s)

    each(0, S, last_end)

    for o in range(1, dpn):
        rows_copy(o, (dpi + dpn - o) % dpn).wait_recv()
    arrived(0, data_kinds)
    for g, left, out_ref in ((1, rows_all, raw1_ref), (0, hid_all, raw2_ref)):
        for i in range(q):
            out_ref[:, i * C : (i + 1) * C] = contract(left[0], g_all[0, g, i])

    def leave(g):
        src, dst = ((raw2_ref, raw2_out), (raw1_ref, raw1_out))[g]
        return fetch(src, dst, sem_l.at[g])

    squares = jnp.zeros((8, 128), F32)
    for g, left, out_ref in ((0, hid_all, raw2_ref), (1, rows_all, raw1_ref)):
        arrived(1, [1] + first_kinds if g == 0 else [0] + last_kinds)
        for i in range(q):
            at = slice(i * C, (i + 1) * C)
            raw = out_ref[:, at] + contract(left[1], g_all[1, g, i])
            out_ref[:, at] = raw
            squares += folded(raw * raw)
        leave(g).start()
    own_stat[1] = squares
    gap = energy[S] - energy[0]
    for s in range(1, S):
        gap += energy[S + s] - energy[s]
    own_stat[0] = gap

    each(0, S, settle)
    for half in range(2):
        exchange_settle(half)
    for w in range(2):
        weight_settle(w)
    for oz in range(1, Z):
        read_copy(oz, z).wait_send()
    for s in range(S):
        give_state(s, a).wait_send()
        give_data(s, a).wait_send()
        for t in range(steps):
            give_noise(t, s, a).wait_send()
    for o in range(1, dpn):
        rows_copy(o, dpi).wait_send()
    first_settle()

    base = 0
    for axis, count, peer in (("fsdp", X, x_peer), ("fsdp", Z, z_peer), ("dp", dpn, dp_peer)):
        copies = []
        for o in range(1, count):
            at = base + o - 1
            copy = send(own_stat, got_stat.at[at], sem_ts.at[at], sem_tr.at[at], {axis: peer(o)})
            copy.start()
            copies.append(copy)
        total = own_stat[...]
        for o, copy in enumerate(copies):
            copy.wait()
            total += got_stat[base + o]
        own_stat[...] = total
        base += count - 1
    total = own_stat[...]
    gap = jnp.sum(total[0], axis=(0, 1), keepdims=True)
    mean = jnp.sum(total[1], axis=(0, 1), keepdims=True) / (2.0 * (C * n) * H)
    stat_ref[0] = jnp.broadcast_to(gap, (8, 128))
    stat_ref[1] = jnp.broadcast_to(1.0 / jnp.sqrt(mean + 1e-06), (8, 128))
    for g in range(2):
        leave(g).wait()


def solution(mesh):
    n, dpn = mesh.shape["fsdp"], mesh.shape["dp"]
    X = inner_of(n)
    Z = n // X
    K = Z // 2
    Y = dpn // 2
    q = n // dpn

    def local(data, start, noise, w1, w2, readout):
        R, C = start.shape
        H = w1.shape[1]
        steps = noise.shape[0]
        S = 2 if R % 64 == 0 else 1
        T = 2 * S
        h = R // T
        vmem = pl.BlockSpec(memory_space=pltpu.VMEM)
        hbm = pl.BlockSpec(memory_space=pl.ANY)
        dma = pltpu.SemaphoreType.DMA
        kinds = 2 + 2 * q
        others = 2 * dpn - 1
        peers = (X - 1) + (Z - 1) + (dpn - 1)
        wide = 2 * C
        X1, K1, Y1 = max(X - 1, 1), max(K - 1, 1), max(Y - 1, 1)
        raw1, raw2, stat = pl.pallas_call(
            functools.partial(kernel, n, X, dpn, steps, S),
            name="contrastive",
            out_shape=(
                jax.ShapeDtypeStruct((C, q * C), F32),
                jax.ShapeDtypeStruct((C, q * C), F32),
                jax.ShapeDtypeStruct((2, 8, 128), F32),
            ),
            in_specs=[hbm] * 5 + [vmem],
            out_specs=(hbm, hbm, vmem),
            scratch_shapes=[
                pltpu.VMEM((C, q * C), F32),
                pltpu.VMEM((C, q * C), F32),
                pltpu.VMEM((wide, H), BF16),
                pltpu.VMEM((wide, H), BF16),
                pltpu.VMEM((2, 2, S, h, C), BF16),
                pltpu.VMEM((2, S, h, C), F32),
                pltpu.VMEM((1, K, X1, R, wide), BF16),
                pltpu.VMEM((1, K, X1, R, wide), BF16),
                pltpu.VMEM((1, K, R, wide), F32),
                pltpu.VMEM((1, K, 2, S * h, wide), BF16),
                pltpu.VMEM((1, K, 2, S * h, wide), BF16),
                pltpu.VMEM((S, h, wide), F32),
                pltpu.VMEM((steps, S, h, wide), F32),
                pltpu.VMEM((T, h, wide), BF16),
                pltpu.VMEM((T, h, wide), BF16),
                pltpu.VMEM((T, h, wide), F32),
                pltpu.VMEM((T, K, h, wide), F32),
                pltpu.VMEM((T, h, wide), F32),
                pltpu.VMEM((Z, 1, C), F32),
                pltpu.VMEM((T, 2, K, X1, h, wide), BF16),
                pltpu.VMEM((T, 2, K, X1, h, wide), BF16),
                pltpu.VMEM((T, 2 * K - 1, h, wide), BF16),
                pltpu.VMEM((T, K1, 1 + K, h, wide), BF16),
                pltpu.VMEM((T, 2, K * X, h, wide), BF16),
                pltpu.VMEM((2, dpn, 2, S, h, C), BF16),
                pltpu.VMEM((2, dpn, 2, S, h, C), BF16),
                pltpu.VMEM((2, 2, q, dpn, 2, S, h, C), BF16),
                pltpu.VMEM((T, 8, 128), F32),
                pltpu.VMEM((2, 8, 128), F32),
                pltpu.VMEM((peers, 2, 8, 128), F32),
                dma((2 + 6 * S,)),
                dma((1, K, X1)), dma((1, K, X1)),
                dma((1, K, 2)), dma((1, K, 2)),
                dma((T,)), dma((T,)),
                dma((steps, S)), dma((steps, S)),
                dma((Z - 1,)), dma((Z - 1,)),
                dma((2, PIECES)), dma((2, PIECES)),
                dma((2, PIECES, Y1)), dma((2, PIECES, Y1)),
                dma((2, PIECES, Y)), dma((2, PIECES, Y)),
                dma((T, 2, K, X1)), dma((T, 2, K, X1)),
                dma((T, K1, 1 + K)), dma((T, K1, 1 + K)),
                dma((T, K1)), dma((T, K1)),
                dma((T, 2, K, X1)), dma((T, 2, K, X1)),
                dma((2, kinds, others, S)), dma((2, kinds, others, S)),
                dma((peers,)), dma((peers,)),
            ],
            compiler_params=pltpu.CompilerParams(
                collective_id=0, has_side_effects=True, vmem_limit_bytes=60 * 1024 * 1024
            ),
        )(data, start, noise, w1, w2, readout.reshape(1, C))
        energy_gap = stat[0, 0, 0] / (R * dpn * 80.0 * jnp.sqrt(jnp.float32(H)))
        return raw1 * stat[1, 0, 0], raw2 * stat[1, 0, 0], energy_gap

    in_specs = (
        P("dp", "fsdp"),
        P("dp", "fsdp"),
        P(None, "dp", "fsdp"),
        P("fsdp", None),
        P("fsdp", None),
        P("fsdp"),
    )
    out_specs = (P("fsdp", "dp"), P("fsdp", "dp"), P())
    return jax.shard_map(local, mesh=mesh, in_specs=in_specs, out_specs=out_specs, check_vma=False)
```
